16 devices in a mesh: rep: 1, dp: 16 (over x, y, z, core).
Axes of the slice: x: 2, y: 2, z: 2, core: 2. Of those that a mesh axis runs over, the one named last changes fastest.
Arguments:
- x: bfloat16 [16, 2048, 1536], P(('rep', 'dp'))
- dy: bfloat16 [16, 2048, 1536], P(('rep', 'dp'))
- w_gate: bfloat16 [2, 1536, 4096], replicated
- w_up: bfloat16 [2, 1536, 4096], replicated
- w_down: bfloat16 [2, 4096, 1536], replicated
- m_w_gate: float32 [2, 1536, 4096], P(None, 'dp')
- m_w_up: float32 [2, 1536, 4096], P(None, 'dp')
- m_w_down: float32 [2, 4096, 1536], P(None, 'dp')
- v_w_gate: float32 [2, 1536, 4096], P(None, 'dp')
- v_w_up: float32 [2, 1536, 4096], P(None, 'dp')
- v_w_down: float32 [2, 4096, 1536], P(None, 'dp')
Outputs:
- output 1: bfloat16 [2, 1536, 4096], P('rep')
- output 2: bfloat16 [2, 1536, 4096], P('rep')
- output 3: bfloat16 [2, 4096, 1536], P('rep')
- output 4: float32 [2, 1536, 4096], P('rep', 'dp')
- output 5: float32 [2, 1536, 4096], P('rep', 'dp')
- output 6: float32 [2, 4096, 1536], P('rep', 'dp')
- output 7: float32 [2, 1536, 4096], P('rep', 'dp')
- output 8: float32 [2, 1536, 4096], P('rep', 'dp')
- output 9: float32 [2, 4096, 1536], P('rep', 'dp')
All inputs are finite; a program needn't handle non-finite values.
Results may differ from the reference program's by a relative error of at most 0.02.
Values are sent between devices in bfloat16 or wider.
A program may use at most 2 GiB of HBM per device.

```python
import jax
import jax.numpy as jnp
from jax import lax

SEQUENCES = 16
TOKENS = 2048
D = 1536
FF = 4096
LAYERS = 2
NAMES = ("w_gate", "w_up", "w_down")
SHAPES = {"w_gate": (LAYERS, D, FF), "w_up": (LAYERS, D, FF), "w_down": (LAYERS, FF, D)}


def bump(key, n, height):
    away = (jnp.arange(n, dtype=jnp.int32) - jax.random.randint(key, (), 0, n, jnp.int32)) % n
    return jnp.where(away < n // 8, height, 1.0)


def together(key, own, strength):
    shared = jax.random.normal(key, own.shape[1:], jnp.float32)
    return (own + strength * shared) * lax.rsqrt(1 + strength * strength)


def setup_inputs(seed: int = 0, part: int = 0) -> dict:
    kx, kdy, ka, kb, kz, kf, kh, kl, *keys = jax.random.split(jax.random.key(seed), 8 + 3 * len(NAMES))
    kx, kdy, ka, kb = (jax.random.fold_in(k, part) for k in (kx, kdy, ka, kb))
    kw, km, kv = (keys[i::3] for i in range(3))
    shape = (SEQUENCES, TOKENS, D)
    much_x, much_dy = jax.random.uniform(kz, (2,), jnp.float32, 0.0, 1.0)
    loud = 2.0 ** jax.random.uniform(jax.random.fold_in(kz, 1), (), jnp.float32, -1.0, 2.0)
    layers = 2.0 ** jax.random.uniform(kl, (LAYERS, 1, 1), jnp.float32, -1.0, 1.0)
    x = together(ka, jax.random.normal(kx, shape, jnp.float32), much_x) * bump(kf, D, 4.0)
    dy = together(kb, jax.random.normal(kdy, shape, jnp.float32), much_dy)
    drawn = {"x": x.astype(jnp.bfloat16), "dy": (loud * dy * (SEQUENCES * TOKENS) ** -0.5).astype(jnp.bfloat16)}
    for key, name in zip(kw, NAMES, strict=True):
        w = jax.random.normal(key, SHAPES[name], jnp.float32) * SHAPES[name][1] ** -0.5
        drawn[name] = (w * {"w_gate": 1.0, "w_up": bump(kh, FF, 4.0), "w_down": layers}[name]).astype(jnp.bfloat16)
    for key, name in zip(km, NAMES, strict=True):
        drawn[f"m_{name}"] = 0.1 * jax.random.normal(key, SHAPES[name], jnp.float32)
    for key, name in zip(kv, NAMES, strict=True):
        drawn[f"v_{name}"] = jax.random.uniform(key, SHAPES[name], jnp.float32, 0.005, 0.015)
    return drawn


def matmul(a, w):
    return jnp.dot(a, w, preferred_element_type=jnp.float32).astype(jnp.bfloat16)


def normed(h):
    wide = h.astype(jnp.float32)
    scale = lax.rsqrt(jnp.mean(wide**2, -1, keepdims=True) + 1e-6)
    return (wide * scale).astype(jnp.bfloat16)


def layer(h, w):
    a = normed(h)
    gate = jnp.dot(a, w["w_gate"], preferred_element_type=jnp.float32)
    up = jnp.dot(a, w["w_up"], preferred_element_type=jnp.float32)
    return h + matmul((jax.nn.silu(gate) * up).astype(jnp.bfloat16), w["w_down"])


def adamw(w, m, v, g):
    m = 0.9 * m + 0.1 * g
    v = 0.95 * v + 0.05 * g * g
    step = m * lax.rsqrt(v + 1e-8) + 0.1 * w
    return (w - 0.02 * step).astype(jnp.bfloat16), m, v


def stack(weights, h):
    return lax.scan(lambda h, w: (layer(h, w), None), h, weights)[0]


def reference(x, dy, w_gate, w_up, w_down, m_w_gate, m_w_up, m_w_down, v_w_gate, v_w_up, v_w_down):
    weights = dict(zip(NAMES, (w_gate, w_up, w_down), strict=True))

    def take(so_far, sequence):
        h, by_y = sequence
        _, back = jax.vjp(lambda w: stack(w, h), weights)
        return jax.tree.map(lambda total, term: total + term.astype(jnp.float32), so_far, back(by_y)[0]), None

    none_yet = {name: jnp.zeros(w.shape, jnp.float32) for name, w in weights.items()}
    by_weights, _ = lax.scan(take, none_yet, (x, dy))
    gradients = [by_weights[name].astype(jnp.bfloat16).astype(jnp.float32) for name in NAMES]
    new = [
        adamw(w.astype(jnp.float32), m, v, g)
        for w, m, v, g in zip((w_gate, w_up, w_down), (m_w_gate, m_w_up, m_w_down), (v_w_gate, v_w_up, v_w_down), gradients, strict=True)
    ]
    return tuple(one[which] for which in range(3) for one in new)
```

```python
import functools

import jax
import jax.numpy as jnp
from jax import lax
from jax.experimental import pallas as pl
from jax.experimental.pallas import tpu as pltpu
from jax.sharding import PartitionSpec as P

BF16, F32 = jnp.bfloat16, jnp.float32
BOTH = ("rep", "dp")
MESH = pl.DeviceIdType.MESH


def dot(a, b, ca, cb):
    return lax.dot_general(a, b, (((ca,), (cb,)), ((), ())), preferred_element_type=F32)


def scale_of(h):
    return lax.rsqrt(jnp.mean(h.astype(F32) ** 2, -1, keepdims=True) + 1e-6)


def hidden(gate, up):
    return (jax.nn.silu(gate) * up).astype(BF16)


def back_hidden(gate, up, by_act):
    by_act = by_act.astype(F32)
    s = jax.nn.sigmoid(gate)
    by_gate = by_act * up * (s * (1 + gate * (1 - s)))
    return by_gate.astype(BF16), (by_act * (gate * s)).astype(BF16)


def back_normed(h, scale, by_a):
    wide, by_a = h.astype(F32), by_a.astype(F32)
    by_scale = jnp.sum(by_a * wide, -1, keepdims=True)
    return (by_a * scale - wide * (by_scale * scale**3 / h.shape[-1])).astype(BF16)


ORDERS = ((0, 1, 2), (1, 2, 0), (2, 0, 1))
DOWN, HIDDEN = 8, 16
UNITS = DOWN + HIDDEN
LAG = 2
ARRIVE = 2 * LAG


def backward(save, number, *refs):
    dy_in, at_in, act_in, g_in, u_in, wd_in, out = refs[:7]
    saved, refs = refs[7 : 7 + 2 * save], refs[7 + 2 * save :]
    (dy, at, act, gate, up, wd, by_gate, by_up, whole, r1, s2, k2, r2, s3, k3, r3, s4, k4, r4) = refs[:19]
    loads, act_sem, in_sem, out_sem, send_sem, recv_sem = refs[19:]
    rep, me = lax.axis_index("rep"), lax.axis_index("dp")
    bits = [(me // (8 >> d)) % 2 for d in range(4)]
    near = [(rep, me + (8 >> d) * (1 - 2 * bits[d])) for d in range(4)]
    core = bits[3]

    def load(src, dst, sem):
        return pltpu.make_async_copy(src, dst, sem)

    def act_load(q):
        return load(act_in.at[:, q], act.at[q % 2], act_sem.at[q % 2])

    def hidden_loads(m):
        cols, slot = pl.ds(pl.multiple_of(m * 256, 256), 256), m % 2
        return (
            load(g_in.at[:, cols], gate.at[slot], in_sem.at[0, slot]),
            load(u_in.at[:, cols], up.at[slot], in_sem.at[1, slot]),
            load(wd_in.at[number, cols], wd.at[slot], in_sem.at[2, slot]),
        )

    def saves(m):
        cols, slot = pl.ds(pl.multiple_of(m * 256, 256), 256), m % 2
        return [
            load(src.at[slot], dst.at[:, cols], out_sem.at[i, slot])
            for i, (src, dst) in enumerate(zip((by_gate, by_up), saved))
        ]

    dy_load = load(dy_in, dy, loads.at[0])
    at_load = load(at_in, at, loads.at[1])
    act_load(0).start()
    dy_load.start()
    act_load(1).start()
    at_load.start()
    for one in hidden_loads(0):
        one.start()

    barrier = pltpu.get_barrier_semaphore()
    for neighbour in near:
        pl.semaphore_signal(barrier, inc=1, device_id=neighbour, device_id_type=MESH)
    pl.semaphore_wait(barrier, 4)

    def copy(i, src, dst, k, dim):
        return pltpu.make_async_remote_copy(
            src_ref=src,
            dst_ref=dst,
            send_sem=send_sem.at[i, k % ARRIVE],
            recv_sem=recv_sem.at[i, k % ARRIVE],
            device_id=near[dim],
            device_id_type=MESH,
        )

    def copies(stage, k):
        if stage == 0:
            return [copy(0, whole.at[k % (LAG + 1), :, 1 - core], r1.at[k % ARRIVE], k, 3)]
        src, dst = ((s2, r2), (s3, r3), (s4, r4))[stage - 1]
        return [
            copy(3 * stage - 2 + p, src.at[k % LAG, p], dst.at[k % ARRIVE, p], k, ORDERS[p][stage - 1]) for p in range(3)
        ]

    def take(stage, k):
        old, now, new = k % ARRIVE, k % LAG, k % (LAG + 1)
        for p, dims in enumerate(ORDERS):
            rows = slice(128 * p, 128 * p + 128)
            own = [bits[d] for d in dims]
            if stage == 0:
                for i in (0, 1):
                    for j in (0, 1):
                        for mine in (False, True):
                            at_bits = dict(zip(dims, (own[0] if mine else 1 - own[0], i, j)))
                            chip = at_bits[0] * 4 + at_bits[1] * 2 + at_bits[2]
                            both = whole[new, chip, core, rows].astype(F32) + r1[old, chip, rows].astype(F32)
                            if mine:
                                k2[now, p, i, j] = both
                            else:
                                s2[now, p, i, j] = both.astype(BF16)
            elif stage == 1:
                for j in (0, 1):
                    i = own[1]
                    s3[now, p, j] = (k2[now, p, 1 - i, j] + r2[old, p, 1 - i, j].astype(F32)).astype(BF16)
                    k3[now, p, j] = k2[now, p, i, j] + r2[old, p, i, j].astype(F32)
            elif stage == 2:
                j = own[2]
                s4[now, p] = (k3[now, p, 1 - j] + r3[old, p, 1 - j].astype(F32)).astype(BF16)
                k4[now, p] = k3[now, p, j] + r3[old, p, j].astype(F32)
            else:
                out[k, rows] = (k4[now, p] + r4[old, p].astype(F32)).astype(BF16)

    def step(n, _):
        for stage in (3, 2, 1, 0):
            k = n - 1 - LAG * (stage + 1)

            @pl.when((k >= 0) & (k < UNITS))
            def _():
                for one in copies(stage, k):
                    one.wait()
                take(stage, k)
                if stage < 3:
                    for one in copies(stage + 1, k):
                        one.start()

        @pl.when((n >= 1) & (n <= UNITS))
        def _():
            for one in copies(0, n - 1):
                one.start()

        slot = n % (LAG + 1)

        @pl.when(n < DOWN)
        def _():
            q = n // 2

            @pl.when(n == 0)
            def _():
                dy_load.wait()

            @pl.when(n % 2 == 0)
            def _():
                act_load(q).wait()

            cols = pl.ds(pl.multiple_of((n % 2) * 768, 768), 768)

            def block(b, _):
                rows = act[q % 2, pl.ds(b * 8, 8)].reshape(512, 2048)
                g = jnp.dot(rows, dy[:, cols], preferred_element_type=F32).astype(BF16)
                for i in range(8):
                    for c in range(6):
                        whole[slot, b * 4 + i // 2, i % 2, 64 * c : 64 * c + 64] = g[
                            64 * i : 64 * i + 64, 128 * c : 128 * c + 128
                        ]

            lax.fori_loop(0, 2, block, None)

            @pl.when((n % 2 == 1) & (q < 2))
            def _():
                act_load(q + 2).start()

        @pl.when((n >= DOWN) & (n < UNITS))
        def _():
            m = n - DOWN
            here = m % 2

            @pl.when(m == 0)
            def _():
                at_load.wait()

            for one in hidden_loads(m):
                one.wait()

            @pl.when(m < HIDDEN - 1)
            def _():
                for one in hidden_loads(m + 1):
                    one.start()

            if save:

                @pl.when(m >= 2)
                def _():
                    for one in saves(m - 2):
                        one.wait()

            def tokens(b, _):
                rows = pl.ds(pl.multiple_of(b * 512, 512), 512)
                by_act = lax.dot_general(dy[rows], wd[here], (((1,), (1,)), ((), ())), preferred_element_type=F32)
                by_g, by_u = back_hidden(gate[here, rows], up[here, rows], by_act.astype(BF16))
                by_gate[here, rows] = by_g
                by_up[here, rows] = by_u

            lax.fori_loop(0, 4, tokens, None)

            def block(b, _):
                rows = at[pl.ds(pl.multiple_of(b * 384, 384), 384)]
                for t, src in enumerate((by_gate, by_up)):
                    g = jnp.dot(rows, src[here], preferred_element_type=F32).astype(BF16)
                    for i in range(4):
                        for c in range(2):
                            lo = 192 * t + 96 * c
                            whole[slot, b * 2 + i // 2, i % 2, lo : lo + 96] = g[
                                96 * i : 96 * i + 96, 128 * c : 128 * c + 128
                            ]

            lax.fori_loop(0, 4, block, None)
            if save:
                for one in saves(m):
                    one.start()

    lax.fori_loop(0, UNITS + 1 + 4 * LAG, step, None)
    if save:
        for m in (HIDDEN - 2, HIDDEN - 1):
            for one in saves(m):
                one.wait()


def gradients(number, dy, a, act, gate, up, w_down, save):
    tokens, d = dy.shape
    ff = act.shape[1]
    any_, vmem = pl.BlockSpec(memory_space=pl.ANY), pl.BlockSpec(memory_space=pltpu.VMEM)
    out_shape = [jax.ShapeDtypeStruct((UNITS, 384, 128), BF16)]
    if save:
        out_shape += [jax.ShapeDtypeStruct((tokens, ff), BF16)] * 2

    def block(dtype, *shape):
        return pltpu.VMEM((*shape, 128, 128), dtype)

    out = pl.pallas_call(
        functools.partial(backward, save, number),
        out_shape=out_shape,
        in_specs=[any_] * 6,
        out_specs=[vmem] + [any_] * (2 * save),
        scratch_shapes=[
            pltpu.VMEM((tokens, d), BF16),
            pltpu.VMEM((d, tokens), BF16),
            pltpu.VMEM((2, 16, 64, tokens), BF16),
            pltpu.VMEM((2, tokens, 256), F32),
            pltpu.VMEM((2, tokens, 256), F32),
            pltpu.VMEM((2, 256, d), BF16),
            pltpu.VMEM((2, tokens, 256), BF16),
            pltpu.VMEM((2, tokens, 256), BF16),
            pltpu.VMEM((LAG + 1, 8, 2, 384, 128), BF16),
            pltpu.VMEM((ARRIVE, 8, 384, 128), BF16),
            block(BF16, LAG, 3, 2, 2),
            block(F32, LAG, 3, 2, 2),
            block(BF16, ARRIVE, 3, 2, 2),
            block(BF16, LAG, 3, 2),
            block(F32, LAG, 3, 2),
            block(BF16, ARRIVE, 3, 2),
            block(BF16, LAG, 3),
            block(F32, LAG, 3),
            block(BF16, ARRIVE, 3),
            pltpu.SemaphoreType.DMA((2,)),
            pltpu.SemaphoreType.DMA((2,)),
            pltpu.SemaphoreType.DMA((3, 2)),
            pltpu.SemaphoreType.DMA((2, 2)),
            pltpu.SemaphoreType.DMA((10, ARRIVE)),
            pltpu.SemaphoreType.DMA((10, ARRIVE)),
        ],
        compiler_params=pltpu.CompilerParams(
            collective_id=number, has_side_effects=True, vmem_limit_bytes=66_000_000
        ),
        cost_estimate=pl.CostEstimate(flops=8 * tokens * d * ff, bytes_accessed=200_000_000, transcendentals=tokens * ff),
    )(dy, a.T, act.T.reshape(16, 4, 64, tokens), gate, up, w_down)
    sums = out[0]
    down = sums[:DOWN].reshape(4, 2, 6, 64, 128).transpose(0, 3, 1, 2, 4).reshape(256, d)
    rest = sums[DOWN:].reshape(HIDDEN, 2, 2, 96, 128).transpose(1, 3, 0, 2, 4).reshape(2, 96, ff)
    return (rest[0], rest[1], down), out[1:]


def adamw(w, m, v, g):
    w, g = w.astype(F32), g.astype(F32)
    m = 0.9 * m + 0.1 * g
    v = 0.95 * v + 0.05 * g * g
    step = m * lax.rsqrt(v + 1e-8) + 0.1 * w
    return (w - 0.02 * step).astype(BF16), m, v


def solution(mesh):
    def compute(x, dy, *arrays):
        (wg, wu, wd), m, v = (arrays[i : i + 3] for i in (0, 3, 6))
        x, dy = x[0], dy[0]
        me = lax.axis_index("dp")
        new = [[None, None] for _ in range(3)]


        def finish(number, sums):
            for which, g in enumerate(sums):
                w, (rows, cols) = (wg, wu, wd)[which], g.shape
                own = lax.dynamic_slice(w, (number, me * rows, 0), (1, rows, cols))[0]
                new[which][number] = adamw(own, m[which][number], v[which][number], g)

        def gather(number):
            for which in (2, 0, 1):
                w, *moments = new[which][number]
                w = lax.all_gather(w, "dp", axis=0, tiled=True)
                new[which][number] = (w, *moments)

        s0 = scale_of(x)
        a0 = (x.astype(F32) * s0).astype(BF16)
        g0, u0 = dot(a0, wg[0], 1, 0), dot(a0, wu[0], 1, 0)
        act0 = hidden(g0, u0)
        h = x + dot(act0, wd[0], 1, 0).astype(BF16)
        s1 = scale_of(h)
        a1 = (h.astype(F32) * s1).astype(BF16)
        g1, u1 = dot(a1, wg[1], 1, 0), dot(a1, wu[1], 1, 0)
        sums, (by_g1, by_u1) = gradients(1, dy, a1, hidden(g1, u1), g1, u1, wd, True)
        finish(1, sums)
        ws = [one[1][0] for one in new]
        ws, by_g1, by_u1 = lax.optimization_barrier((ws, by_g1, by_u1))
        for one, w in zip(new, ws):
            one[1] = (w, *one[1][1:])
        gather(1)
        by_a1 = dot(by_g1, wg[1], 1, 1).astype(BF16) + dot(by_u1, wu[1], 1, 1).astype(BF16)
        by_h = dy + back_normed(h, s1, by_a1)
        sums, _ = gradients(0, by_h, a0, act0, g0, u0, wd, False)
        finish(0, sums)
        gather(0)
        return tuple(jnp.stack([one[n][k] for n in range(2)]) for k in range(3) for one in new)

    whole, rows = P(None, None, None), P(None, "dp", None)
    seq = P(BOTH, None, None)
    return jax.shard_map(
        compute,
        mesh=mesh,
        in_specs=(seq, seq, whole, whole, whole) + (rows,) * 6,
        out_specs=(P("rep", None, None),) * 3 + (P("rep", "dp", None),) * 6,
        check_vma=False,
    )
```

```python
import functools

import jax
import jax.numpy as jnp
from jax import lax
from jax.experimental import pallas as pl
from jax.experimental.pallas import tpu as pltpu
from jax.sharding import PartitionSpec as P

BF16, F32 = jnp.bfloat16, jnp.float32
BOTH = ("rep", "dp")
MESH = pl.DeviceIdType.MESH


def scale_of(h):
    return lax.rsqrt(jnp.mean(h.astype(F32) ** 2, -1, keepdims=True) + 1e-6)


def hidden(gate, up):
    return (jax.nn.silu(gate) * up).astype(BF16)


def back_hidden(gate, up, by_act):
    by_act = by_act.astype(F32)
    s = jax.nn.sigmoid(gate)
    by_gate = by_act * up * (s * (1 + gate * (1 - s)))
    return by_gate.astype(BF16), (by_act * (gate * s)).astype(BF16)


def back_normed(h, scale, by_a):
    wide, by_a = h.astype(F32), by_a.astype(F32)
    by_scale = jnp.sum(by_a * wide, -1, keepdims=True)
    return (by_a * scale - wide * (by_scale * scale**3 / h.shape[-1])).astype(BF16)


ORDERS = ((0, 1, 2), (1, 2, 0), (2, 0, 1))
COUNTS = (8, 16)
LAG = 2
ARRIVE = 2 * LAG


def backward(save, number, with_down, with_hidden, *refs):
    DOWN, HIDDEN = COUNTS[0] * with_down, COUNTS[1] * with_hidden
    UNITS = DOWN + HIDDEN
    refs = list(refs)

    def pop(wanted, n):
        return [refs.pop(0) for _ in range(n)] if wanted else [None] * n

    (dy_in,) = pop(True, 1)
    (act_in,) = pop(with_down, 1)
    at_in, g_in, u_in, wd_in = pop(with_hidden, 4)
    (out,) = pop(True, 1)
    saved = pop(save, 2)
    (dy,) = pop(True, 1)
    (act,) = pop(with_down, 1)
    at, gate, up, wd, by_gate, by_up = pop(with_hidden, 6)
    whole, r1, s2, k2, r2, s3, k3, r3, s4, k4, r4 = pop(True, 11)
    loads, act_sem, in_sem, out_sem, send_sem, recv_sem = pop(True, 6)
    rep, me = lax.axis_index("rep"), lax.axis_index("dp")
    bits = [(me // (8 >> d)) % 2 for d in range(4)]
    near = [(rep, me + (8 >> d) * (1 - 2 * bits[d])) for d in range(4)]
    core = bits[3]

    def load(src, dst, sem):
        return pltpu.make_async_copy(src, dst, sem)

    def act_load(q):
        return load(act_in.at[:, q], act.at[q % 2], act_sem.at[q % 2])

    def hidden_loads(m):
        cols, slot = pl.ds(pl.multiple_of(m * 256, 256), 256), m % 2
        return (
            load(g_in.at[:, cols], gate.at[slot], in_sem.at[0, slot]),
            load(u_in.at[:, cols], up.at[slot], in_sem.at[1, slot]),
            load(wd_in.at[number, cols], wd.at[slot], in_sem.at[2, slot]),
        )

    def saves(m):
        cols, slot = pl.ds(pl.multiple_of(m * 256, 256), 256), m % 2
        return [
            load(src.at[slot], dst.at[:, cols], out_sem.at[i, slot])
            for i, (src, dst) in enumerate(zip((by_gate, by_up), saved))
        ]

    dy_load = load(dy_in, dy, loads.at[0])
    if with_down:
        act_load(0).start()
    dy_load.start()
    if with_down:
        act_load(1).start()
    if with_hidden:
        for one in hidden_loads(0):
            one.start()
        at_load = load(at_in, at, loads.at[1])
        at_load.start()

    barrier = pltpu.get_barrier_semaphore()
    for neighbour in near:
        pl.semaphore_signal(barrier, inc=1, device_id=neighbour, device_id_type=MESH)
    pl.semaphore_wait(barrier, 4)

    def copy(i, src, dst, k, dim):
        return pltpu.make_async_remote_copy(
            src_ref=src,
            dst_ref=dst,
            send_sem=send_sem.at[i, k % ARRIVE],
            recv_sem=recv_sem.at[i, k % ARRIVE],
            device_id=near[dim],
            device_id_type=MESH,
        )

    def copies(stage, k):
        if stage == 0:
            return [copy(0, whole.at[k % (LAG + 1), :, 1 - core], r1.at[k % ARRIVE], k, 3)]
        src, dst = ((s2, r2), (s3, r3), (s4, r4))[stage - 1]
        return [
            copy(3 * stage - 2 + p, src.at[k % LAG, p], dst.at[k % ARRIVE, p], k, ORDERS[p][stage - 1]) for p in range(3)
        ]

    def take(stage, k):
        old, now, new = k % ARRIVE, k % LAG, k % (LAG + 1)
        for p, dims in enumerate(ORDERS):
            rows = slice(128 * p, 128 * p + 128)
            own = [bits[d] for d in dims]
            if stage == 0:
                for i in (0, 1):
                    for j in (0, 1):
                        for mine in (False, True):
                            at_bits = dict(zip(dims, (own[0] if mine else 1 - own[0], i, j)))
                            chip = at_bits[0] * 4 + at_bits[1] * 2 + at_bits[2]
                            both = whole[new, chip, core, rows].astype(F32) + r1[old, chip, rows].astype(F32)
                            if mine:
                                k2[now, p, i, j] = both
                            else:
                                s2[now, p, i, j] = both.astype(BF16)
            elif stage == 1:
                for j in (0, 1):
                    i = own[1]
                    s3[now, p, j] = (k2[now, p, 1 - i, j] + r2[old, p, 1 - i, j].astype(F32)).astype(BF16)
                    k3[now, p, j] = k2[now, p, i, j] + r2[old, p, i, j].astype(F32)
            elif stage == 2:
                j = own[2]
                s4[now, p] = (k3[now, p, 1 - j] + r3[old, p, 1 - j].astype(F32)).astype(BF16)
                k4[now, p] = k3[now, p, j] + r3[old, p, j].astype(F32)
            else:
                out[k, rows] = (k4[now, p] + r4[old, p].astype(F32)).astype(BF16)

    def step(n, _):
        for stage in (3, 2, 1, 0):
            k = n - 1 - LAG * (stage + 1)

            @pl.when((k >= 0) & (k < UNITS))
            def _():
                for one in copies(stage, k):
                    one.wait()
                take(stage, k)
                if stage < 3:
                    for one in copies(stage + 1, k):
                        one.start()

        @pl.when((n >= 1) & (n <= UNITS))
        def _():
            for one in copies(0, n - 1):
                one.start()

        slot = n % (LAG + 1)

        @pl.when(n == 0)
        def _():
            dy_load.wait()

        if with_down:
            @pl.when(n < DOWN)
            def _():
                q = n // 2

                @pl.when(n % 2 == 0)
                def _():
                    act_load(q).wait()

                cols = pl.ds(pl.multiple_of((n % 2) * 768, 768), 768)

                def block(b, _):
                    rows = act[q % 2, pl.ds(b * 8, 8)].reshape(512, 2048)
                    g = jnp.dot(rows, dy[:, cols], preferred_element_type=F32).astype(BF16)
                    for i in range(8):
                        for c in range(6):
                            whole[slot, b * 4 + i // 2, i % 2, 64 * c : 64 * c + 64] = g[
                                64 * i : 64 * i + 64, 128 * c : 128 * c + 128
                            ]

                lax.fori_loop(0, 2, block, None)

                @pl.when((n % 2 == 1) & (q < 2))
                def _():
                    act_load(q + 2).start()

        if not with_hidden:
            return

        @pl.when((n >= DOWN) & (n < UNITS))
        def _():
            m = n - DOWN
            here = m % 2

            @pl.when(m == 0)
            def _():
                at_load.wait()

            for one in hidden_loads(m):
                one.wait()

            @pl.when(m < HIDDEN - 1)
            def _():
                for one in hidden_loads(m + 1):
                    one.start()

            if save:

                @pl.when(m >= 2)
                def _():
                    for one in saves(m - 2):
                        one.wait()

            def tokens(b, _):
                rows = pl.ds(pl.multiple_of(b * 512, 512), 512)
                by_act = lax.dot_general(dy[rows], wd[here], (((1,), (1,)), ((), ())), preferred_element_type=F32)
                by_g, by_u = back_hidden(gate[here, rows], up[here, rows], by_act.astype(BF16))
                by_gate[here, rows] = by_g
                by_up[here, rows] = by_u

            lax.fori_loop(0, 4, tokens, None)

            def block(b, _):
                rows = at[pl.ds(pl.multiple_of(b * 384, 384), 384)]
                for t, src in enumerate((by_gate, by_up)):
                    g = jnp.dot(rows, src[here], preferred_element_type=F32).astype(BF16)
                    for i in range(4):
                        for c in range(2):
                            lo = 192 * t + 96 * c
                            whole[slot, b * 2 + i // 2, i % 2, lo : lo + 96] = g[
                                96 * i : 96 * i + 96, 128 * c : 128 * c + 128
                            ]

            lax.fori_loop(0, 4, block, None)
            if save:
                for one in saves(m):
                    one.start()

    lax.fori_loop(0, UNITS + 1 + 4 * LAG, step, None)
    if save:
        for m in (HIDDEN - 2, HIDDEN - 1):
            for one in saves(m):
                one.wait()


def gradients(number, dy, a, act_t, gate, up, w_down, *, save=False, with_down=True, with_hidden=True, collective):
    tokens, d = dy.shape
    ff = w_down.shape[1]
    any_, vmem = pl.BlockSpec(memory_space=pl.ANY), pl.BlockSpec(memory_space=pltpu.VMEM)
    down, hidden_ = COUNTS[0] * with_down, COUNTS[1] * with_hidden
    out_shape = [jax.ShapeDtypeStruct((down + hidden_, 384, 128), BF16)]
    if save:
        out_shape += [jax.ShapeDtypeStruct((tokens, ff), BF16)] * 2

    def block(dtype, *shape):
        return pltpu.VMEM((*shape, 128, 128), dtype)

    operands, scratch = [dy], [pltpu.VMEM((tokens, d), BF16)]
    if with_down:
        operands.append(act_t.reshape(16, 4, 64, tokens))
        scratch.append(pltpu.VMEM((2, 16, 64, tokens), BF16))
    if with_hidden:
        operands += [a.T, gate, up, w_down]
        scratch += [
            pltpu.VMEM((d, tokens), BF16),
            pltpu.VMEM((2, tokens, 256), F32),
            pltpu.VMEM((2, tokens, 256), F32),
            pltpu.VMEM((2, 256, d), BF16),
            pltpu.VMEM((2, tokens, 256), BF16),
            pltpu.VMEM((2, tokens, 256), BF16),
        ]
    out = pl.pallas_call(
        functools.partial(backward, save, number, with_down, with_hidden),
        out_shape=out_shape,
        in_specs=[any_] * len(operands),
        out_specs=[vmem] + [any_] * (2 * save),
        scratch_shapes=scratch
        + [
            pltpu.VMEM((LAG + 1, 8, 2, 384, 128), BF16),
            pltpu.VMEM((ARRIVE, 8, 384, 128), BF16),
            block(BF16, LAG, 3, 2, 2),
            block(F32, LAG, 3, 2, 2),
            block(BF16, ARRIVE, 3, 2, 2),
            block(BF16, LAG, 3, 2),
            block(F32, LAG, 3, 2),
            block(BF16, ARRIVE, 3, 2),
            block(BF16, LAG, 3),
            block(F32, LAG, 3),
            block(BF16, ARRIVE, 3),
            pltpu.SemaphoreType.DMA((2,)),
            pltpu.SemaphoreType.DMA((2,)),
            pltpu.SemaphoreType.DMA((3, 2)),
            pltpu.SemaphoreType.DMA((2, 2)),
            pltpu.SemaphoreType.DMA((10, ARRIVE)),
            pltpu.SemaphoreType.DMA((10, ARRIVE)),
        ],
        compiler_params=pltpu.CompilerParams(
            collective_id=collective, has_side_effects=True, vmem_limit_bytes=66_000_000
        ),
        cost_estimate=pl.CostEstimate(
            flops=(2 * with_down + 6 * with_hidden) * tokens * d * ff,
            bytes_accessed=100_000_000,
            transcendentals=tokens * ff,
        ),
    )(*operands)
    sums, found = out[0], {}
    if with_down:
        found[2] = sums[:down].reshape(4, 2, 6, 64, 128).transpose(0, 3, 1, 2, 4).reshape(256, d)
    if with_hidden:
        rest = sums[down:].reshape(hidden_, 2, 2, 96, 128).transpose(1, 3, 0, 2, 4).reshape(2, 96, ff)
        found[0], found[1] = rest[0], rest[1]
    return found, out[1:]


def forward_hidden(number, a, w_gate, w_up, natural):
    tokens, d = a.shape
    ff, width = w_gate.shape[2], 256

    def kernel(a_ref, wg_ref, wu_ref, gate_ref, up_ref, act_t_ref, *act_ref):
        def block(b, _):
            rows = pl.ds(pl.multiple_of(b * 512, 512), 512)
            gate = jnp.dot(a_ref[rows], wg_ref[0], preferred_element_type=F32)
            up = jnp.dot(a_ref[rows], wu_ref[0], preferred_element_type=F32)
            gate_ref[rows] = gate
            up_ref[rows] = up
            act = hidden(gate, up)
            act_t_ref[:, rows] = act.T
            if natural:
                act_ref[0][rows] = act

        lax.fori_loop(0, tokens // 512, block, None)

    wide = pl.BlockSpec((tokens, width), lambda i: (0, i))
    weight = pl.BlockSpec((1, d, width), lambda i: (number, 0, i))
    outs = [((tokens, ff), F32), ((tokens, ff), F32), ((ff, tokens), BF16)] + [((tokens, ff), BF16)] * natural
    return pl.pallas_call(
        kernel,
        grid=(ff // width,),
        out_shape=[jax.ShapeDtypeStruct(*one) for one in outs],
        in_specs=[pl.BlockSpec((tokens, d), lambda i: (0, 0)), weight, weight],
        out_specs=[wide, wide, pl.BlockSpec((width, tokens), lambda i: (i, 0))] + [wide] * natural,
        compiler_params=pltpu.CompilerParams(vmem_limit_bytes=60_000_000),
        cost_estimate=pl.CostEstimate(
            flops=4 * tokens * d * ff, bytes_accessed=130_000_000, transcendentals=tokens * ff
        ),
    )(a, w_gate, w_up)


def forward_down(number, x, act, w_down):
    tokens, d = x.shape
    ff, height = act.shape[1], 512

    def kernel(x_ref, act_ref, wd_ref, h_ref, s_ref, a_ref):
        for c in range(0, d, 512):
            cols = slice(c, c + 512)
            out = jnp.dot(act_ref[...], wd_ref[0, :, cols], preferred_element_type=F32).astype(BF16)
            h_ref[:, cols] = x_ref[:, cols] + out
        wide = h_ref[...].astype(F32)
        scale = lax.rsqrt(jnp.mean(wide**2, -1, keepdims=True) + 1e-6)
        s_ref[...] = scale
        a_ref[...] = (wide * scale).astype(BF16)

    def rows(n):
        return pl.BlockSpec((height, n), lambda i: (i, 0))

    return pl.pallas_call(
        kernel,
        name="forward_down",
        grid=(tokens // height,),
        out_shape=[
            jax.ShapeDtypeStruct((tokens, d), BF16),
            jax.ShapeDtypeStruct((tokens, 1), F32),
            jax.ShapeDtypeStruct((tokens, d), BF16),
        ],
        in_specs=[rows(d), rows(ff), pl.BlockSpec((1, ff, d), lambda i: (number, 0, 0), pipeline_mode=pl.Buffered(1))],
        out_specs=[rows(d), rows(1), rows(d)],
        compiler_params=pltpu.CompilerParams(vmem_limit_bytes=60_000_000),
        cost_estimate=pl.CostEstimate(flops=2 * tokens * d * ff, bytes_accessed=50_000_000, transcendentals=tokens),
    )(x, act, w_down)


def back_layer(number, by_gate, by_up, w_gate, w_up, h, scale, dy):
    tokens, d = h.shape
    ff, height = by_gate.shape[1], 512

    def kernel(g_ref, u_ref, wg_ref, wu_ref, h_ref, s_ref, dy_ref, out_ref, by_a):
        def part(c, _):
            cols = pl.ds(pl.multiple_of(c * 512, 512), 512)
            terms = [
                lax.dot_general(t[...], w[0, cols], (((1,), (1,)), ((), ())), preferred_element_type=F32).astype(BF16)
                for t, w in ((g_ref, wg_ref), (u_ref, wu_ref))
            ]
            by_a[:, cols] = terms[0] + terms[1]

        lax.fori_loop(0, d // 512, part, None)
        out_ref[...] = dy_ref[...] + back_normed(h_ref[...], s_ref[...], by_a[...])

    def rows(n):
        return pl.BlockSpec((height, n), lambda i: (i, 0))

    weight = pl.BlockSpec((1, d, ff), lambda i: (number, 0, 0), pipeline_mode=pl.Buffered(1))
    return pl.pallas_call(
        kernel,
        name="back_layer",
        grid=(tokens // height,),
        out_shape=jax.ShapeDtypeStruct((tokens, d), BF16),
        in_specs=[rows(ff), rows(ff), weight, weight, rows(d), rows(1), rows(d)],
        out_specs=rows(d),
        scratch_shapes=[pltpu.VMEM((height, d), BF16)],
        compiler_params=pltpu.CompilerParams(vmem_limit_bytes=64_000_000),
        cost_estimate=pl.CostEstimate(flops=4 * tokens * d * ff, bytes_accessed=80_000_000, transcendentals=tokens),
    )(by_gate, by_up, w_gate, w_up, h, scale, dy)


def adamw(w, m, v, g):
    w, g = w.astype(F32), g.astype(F32)
    m = 0.9 * m + 0.1 * g
    v = 0.95 * v + 0.05 * g * g
    step = m * lax.rsqrt(v + 1e-8) + 0.1 * w
    return (w - 0.02 * step).astype(BF16), m, v


def solution(mesh):
    def compute(x, dy, *arrays):
        (wg, wu, wd), m, v = (arrays[i : i + 3] for i in (0, 3, 6))
        x, dy = x[0], dy[0]
        me = lax.axis_index("dp")
        new = [[None, None] for _ in range(3)]


        def finish(number, sums):
            for which, g in sums.items():
                w, (rows, cols) = (wg, wu, wd)[which], g.shape
                own = lax.dynamic_slice(w, (number, me * rows, 0), (1, rows, cols))[0]
                new[which][number] = adamw(own, m[which][number], v[which][number], g)

        def gather(number, *names):
            for which in names:
                w, *moments = new[which][number]
                w = lax.all_gather(w, "dp", axis=0, tiled=True)
                new[which][number] = (w, *moments)

        def first(number, names, others):
            ws, others = lax.optimization_barrier(([new[which][number][0] for which in names], others))
            for which, w in zip(names, ws):
                new[which][number] = (w, *new[which][number][1:])
            gather(number, *names)
            return others

        a0 = (x.astype(F32) * scale_of(x)).astype(BF16)
        g0, u0, act0_t, act0 = forward_hidden(0, a0, wg, wu, True)
        h, s1, a1 = forward_down(0, x, act0, wd)
        g1, u1, act1_t = forward_hidden(1, a1, wg, wu, False)
        sums, by_hidden = gradients(1, dy, a1, act1_t, g1, u1, wd, save=True, collective=1)
        finish(1, sums)
        by_hidden = first(1, (2, 0, 1), by_hidden)
        by_h = back_layer(1, *by_hidden, wg, wu, h, s1, dy)
        sums, _ = gradients(0, by_h, None, act0_t, None, None, wd, with_hidden=False, collective=2)
        finish(0, sums)
        by_h = first(0, (2,), by_h)
        sums, _ = gradients(0, by_h, a0, None, g0, u0, wd, with_down=False, collective=3)
        finish(0, sums)
        gather(0, 0, 1)
        return tuple(jnp.stack([one[n][k] for n in range(2)]) for k in range(3) for one in new)

    whole, rows = P(None, None, None), P(None, "dp", None)
    seq = P(BOTH, None, None)
    return jax.shard_map(
        compute,
        mesh=mesh,
        in_specs=(seq, seq, whole, whole, whole) + (rows,) * 6,
        out_specs=(P("rep", None, None),) * 3 + (P("rep", "dp", None),) * 6,
        check_vma=False,
    )
```
